32 devices in a mesh: groups: 2 (over y), tm: 8 (over z, x), space: 2 (over core).
Axes of the slice: x: 2, y: 2, z: 4, core: 2. Of those that a mesh axis runs over, the one named last changes fastest.
Arguments:
- iterate: float32 [16, 16, 16, 128], P(('groups', 'tm'), 'space'), parts along dimension 0, may hold values from -0.7 to 1.3
- source: float32 [16, 16, 16, 128], P(('groups', 'tm'), 'space'), parts along dimension 0, may hold values from -6 to 6
- diffusivity: float32 [32, 16, 128], P(('groups', 'space')), parts along dimension 0, may hold values from 0.1 to 1
Outputs:
- new_iterate: float32 [16, 16, 16, 128], P(('groups', 'tm'), 'space'), parts along dimension 0
- new_residual: float32 [16, 16, 16, 128], P(('groups', 'tm'), 'space'), parts along dimension 0
The draws below stay inside these ranges and needn't reach their ends.
There are 2 independent parts, one for each index of `groups`. The reference program is written for one: setup_inputs(seed, part) draws one part's arguments, and reference() takes and returns one part's arrays. A program takes and returns all parts, laid end to end along the dimension named above; each array names one. Nothing has to cross between parts.
All inputs are finite; a program needn't handle non-finite values.
Results may differ from the reference program's by a relative error of at most 0.0019.
Values sent between devices are 32-bit elements; how exact they have to be, the bound alone decides.
A program may use at most 64 MiB of HBM per device.

```python
import math
import jax
import jax.numpy as jnp
from jax import lax

NX = 128
NY = 16
SWEEPS = 6
NT = 8
NZ = 16


def draw_iterate(key, part):
    shape = (NT, NZ, NY, NX)
    values = 0.3 + 0.25 * jax.random.normal(key, shape, jnp.float32)
    return jnp.clip(values, -0.7, 1.3)


def block_scale(rng, shape, split, low, high):
    level = 1.0
    for dim, parts in split:
        draws = jax.random.uniform(jax.random.fold_in(jax.random.fold_in(rng, 6), dim), (parts,), jnp.float32, low / len(split), high / len(split))
        level = level * jnp.repeat(jnp.exp(draws), shape[dim] // parts).reshape((-1,) + (1,) * (len(shape) - 1 - dim))
    return level


def gaussian(key, dims, spread, most, shards=(), held_as=jnp.bfloat16):
    values = jax.random.normal(key, dims, jnp.float32) * spread
    if len(shards) > 0:
        values = block_scale(key, dims, shards, -0.22, 0.18) * values
    return jnp.clip(values, min=-most, max=most).astype(held_as)


def setup_inputs(seed: int = 0, part: int = 0) -> dict:
    arg_keys = jax.random.split(jax.random.key(seed), 4)
    part_keys = jax.random.split(jax.random.fold_in(arg_keys[3], part), 4)
    return {
        "iterate": draw_iterate(jax.random.fold_in(jax.random.fold_in(arg_keys[3], part), 71), part),
        "source": gaussian(part_keys[1], (NT, NZ, NY, NX), 1.0, 6.0, ((0, 8), (1, 2)), jnp.float32),
        "diffusivity": jnp.clip(jnp.exp(math.log(1.0) - 2.3025851 * jax.random.uniform(part_keys[2], (NZ, NY, NX), jnp.float32) ** block_scale(part_keys[2], (NZ, NY, NX), ((0, 2),), -0.2, 0.2)), 0.1, 1.0),
    }


frac_order = 0.3
step_length = 0.01
gamma_factor = 0.9086387328532904


def history_weights(lags):
    scale = 1.0 / (step_length ** frac_order * gamma_factor)
    power = 1.0 - frac_order
    safe = jnp.maximum(lags, 0.0)
    upper = (safe + 1.0) ** power - safe ** power
    lower = jnp.where(safe >= 1.0, safe ** power - jnp.maximum(safe - 1.0, 0.0) ** power, 0.0)
    return jnp.where(lags >= 0.0, (upper - lower) * scale, 0.0)


def circulant_spectrum(freqs, total):
    lags = jnp.arange(total, dtype=jnp.int32)
    first = jnp.where(lags < total // 2, history_weights(lags.astype(jnp.float32)), 0.0)
    phase = ((freqs[:, None] * lags[None, :]) % total).astype(jnp.float32) * (2.0 * math.pi / total)
    real_part = jnp.sum(first[None, :] * jnp.cos(phase), axis=1)
    imag_part = -jnp.sum(first[None, :] * jnp.sin(phase), axis=1)
    return real_part, imag_part


def fourier_tables(total):
    index = jnp.arange(total, dtype=jnp.int32)
    phase = ((index[:, None] * index[None, :]) % total).astype(jnp.float32) * (2.0 * math.pi / total)
    return jnp.cos(phase), jnp.sin(phase)


def neighbour_sum(padded):
    inner = padded[..., 1:-1, :, :]
    result = padded[..., 2:, :, :] + padded[..., :-2, :, :]
    along_y = jnp.pad(inner, [(0, 0)] * (inner.ndim - 2) + [(1, 1), (0, 0)])
    result = result + along_y[..., 2:, :] + along_y[..., :-2, :]
    along_x = jnp.pad(inner, [(0, 0)] * (inner.ndim - 1) + [(1, 1)])
    return result + along_x[..., 2:] + along_x[..., :-2]


def jacobi_step(spec_re, spec_im, sol_re, sol_im, stiff_re, stiff_im, lam_re, lam_im, inv_re, inv_im):
    res_re = spec_re - (lam_re * sol_re - lam_im * sol_im) - stiff_re
    res_im = spec_im - (lam_re * sol_im + lam_im * sol_re) - stiff_im
    return sol_re + (res_re * inv_re - res_im * inv_im), sol_im + (res_re * inv_im + res_im * inv_re)


def stiffness(field, diffusivity):
    padded = jnp.pad(field, ((0, 0), (1, 1), (0, 0), (0, 0)))
    return diffusivity * (6.0 * field - neighbour_sum(padded))


def apply_time(matrix, field):
    steps = field.shape[0]
    flat = field.reshape(steps, -1)
    return jnp.dot(matrix, flat, precision=lax.Precision.HIGHEST).reshape(field.shape)


def reference(iterate, source, diffusivity):
    total = iterate.shape[0]
    times = jnp.arange(total, dtype=jnp.int32)
    toeplitz = history_weights((times[:, None] - times[None, :]).astype(jnp.float32))
    stiff_iter = stiffness(iterate, diffusivity)
    residual = source - apply_time(toeplitz, iterate) - stiff_iter
    cos_table, sin_table = fourier_tables(total)
    spec_re = apply_time(cos_table, residual)
    spec_im = -apply_time(sin_table, residual)
    lam_re, lam_im = circulant_spectrum(times, total)
    lam_re = lam_re[:, None, None, None]
    lam_im = lam_im[:, None, None, None]
    diag_re = lam_re + 6.0 * diffusivity
    denom = diag_re * diag_re + lam_im * lam_im
    inv_re = diag_re / denom
    inv_im = -lam_im / denom
    sol_re = spec_re * inv_re - spec_im * inv_im
    sol_im = spec_re * inv_im + spec_im * inv_re
    for sweep in range(SWEEPS - 1):
        stiff_re = stiffness(sol_re, diffusivity)
        stiff_im = stiffness(sol_im, diffusivity)
        sol_re, sol_im = jacobi_step(spec_re, spec_im, sol_re, sol_im, stiff_re, stiff_im, lam_re, lam_im, inv_re, inv_im)
    stiff_re = stiffness(sol_re, diffusivity)
    stiff_im = stiffness(sol_im, diffusivity)
    correction = (apply_time(cos_table, sol_re) - apply_time(sin_table, sol_im)) / total
    stiff_time = (apply_time(cos_table, stiff_re) - apply_time(sin_table, stiff_im)) / total
    image = apply_time(toeplitz, correction) + stiff_time
    step = jnp.sum(residual * image) / jnp.sum(image * image)
    return iterate + step * correction, residual - step * image
```

```python
import functools
import math

import jax
import jax.numpy as jnp
from jax import lax
from jax.experimental import pallas as pl
from jax.experimental.pallas import tpu as pltpu
from jax.sharding import PartitionSpec as P

SWEEPS = 6


frac_order = 0.3
step_length = 0.01
gamma_factor = 0.9086387328532904


def with_halo(value, sides, width):
    for axis, dim in sides:
        peers, length = (lax.axis_size(axis), value.shape[dim])
        up = [(i, (i + 1) % peers) for i in range(peers - 1)]
        down = [(j, i) for i, j in up]
        last = lax.slice_in_dim(value, length - width, length, axis=dim)
        first = lax.slice_in_dim(value, 0, width, axis=dim)
        before = lax.ppermute(last, axis, up)
        after = lax.ppermute(first, axis, down)
        value = jnp.concatenate([before, value, after], axis=dim)
    return value


def history_weights(lags):
    scale = 1.0 / (step_length**frac_order * gamma_factor)
    power = 1.0 - frac_order
    safe = jnp.maximum(lags, 0.0)
    upper = (safe + 1.0) ** power - safe**power
    lower = jnp.where(safe >= 1.0, safe**power - jnp.maximum(safe - 1.0, 0.0) ** power, 0.0)
    return jnp.where(lags >= 0.0, (upper - lower) * scale, 0.0)


def circulant_spectrum(freqs, total):
    lags = jnp.arange(total, dtype=jnp.int32)
    first = jnp.where(lags < total // 2, history_weights(lags.astype(jnp.float32)), 0.0)
    phase = (freqs[:, None] * lags[None, :] % total).astype(jnp.float32) * (2.0 * math.pi / total)
    real_part = jnp.sum(first[None, :] * jnp.cos(phase), axis=1)
    imag_part = -jnp.sum(first[None, :] * jnp.sin(phase), axis=1)
    return (real_part, imag_part)


def fourier_tables(total):
    index = jnp.arange(total, dtype=jnp.int32)
    phase = (index[:, None] * index[None, :] % total).astype(jnp.float32) * (2.0 * math.pi / total)
    return (jnp.cos(phase), jnp.sin(phase))


def neighbour_sum(padded):
    inner = padded[..., 1:-1, :, :]
    result = padded[..., 2:, :, :] + padded[..., :-2, :, :]
    along_y = jnp.pad(inner, [(0, 0)] * (inner.ndim - 2) + [(1, 1), (0, 0)])
    result = result + along_y[..., 2:, :] + along_y[..., :-2, :]
    along_x = jnp.pad(inner, [(0, 0)] * (inner.ndim - 1) + [(1, 1)])
    return result + along_x[..., 2:] + along_x[..., :-2]


def jacobi_step(
    spec_re, spec_im, sol_re, sol_im, stiff_re, stiff_im, lam_re, lam_im, inv_re, inv_im
):
    res_re = spec_re - (lam_re * sol_re - lam_im * sol_im) - stiff_re
    res_im = spec_im - (lam_re * sol_im + lam_im * sol_re) - stiff_im
    return (
        sol_re + (res_re * inv_re - res_im * inv_im),
        sol_im + (res_re * inv_im + res_im * inv_re),
    )


def stiffness_pair(sol_re, sol_im, diffusivity):
    stacked = jnp.stack([sol_re, sol_im])
    padded = with_halo(stacked, (("space", 2),), 1)
    stiff = diffusivity * (6.0 * stacked - neighbour_sum(padded))
    return (stiff[0], stiff[1])


def time_product(matrix, field):
    return jnp.dot(matrix, field, precision=lax.Precision.HIGHEST)


def inner_products(residual, image):
    return lax.psum((jnp.sum(residual * image), jnp.sum(image * image)), ("tm", "space"))


def on_device(iterate, source, diffusivity):
    steps_here = iterate.shape[0]
    slab_shape = iterate.shape
    cells = slab_shape[1] * slab_shape[2] * slab_shape[3]
    total = steps_here * lax.axis_size("tm")
    my_times = lax.axis_index("tm") * steps_here + jnp.arange(steps_here, dtype=jnp.int32)
    times = jnp.arange(total, dtype=jnp.int32)
    toeplitz = history_weights((times[:, None] - times[None, :]).astype(jnp.float32))
    cos_table, sin_table = fourier_tables(total)
    padded = with_halo(iterate, (("space", 1),), 1)
    stiff_iter = diffusivity * (6.0 * iterate - neighbour_sum(padded))
    flat_iter = iterate.reshape(steps_here, cells)
    flat_source = source.reshape(steps_here, cells)
    flat_stiff = stiff_iter.reshape(steps_here, cells)
    iter_cols, source_cols, stiff_cols = (
        lax.all_to_all(flat_iter, "tm", split_axis=1, concat_axis=0, tiled=True),
        lax.all_to_all(flat_source, "tm", split_axis=1, concat_axis=0, tiled=True),
        lax.all_to_all(flat_stiff, "tm", split_axis=1, concat_axis=0, tiled=True),
    )
    residual = source_cols - time_product(toeplitz, iter_cols) - stiff_cols
    spec_re = time_product(cos_table, residual)
    spec_im = -time_product(sin_table, residual)
    spec_re, spec_im = (
        lax.all_to_all(spec_re, "tm", split_axis=0, concat_axis=1, tiled=True),
        lax.all_to_all(spec_im, "tm", split_axis=0, concat_axis=1, tiled=True),
    )
    spec_re = spec_re.reshape(slab_shape)
    spec_im = spec_im.reshape(slab_shape)
    lam_re, lam_im = circulant_spectrum(my_times, total)
    lam_re = lam_re[:, None, None, None]
    lam_im = lam_im[:, None, None, None]
    diag_re = lam_re + 6.0 * diffusivity
    denom = diag_re * diag_re + lam_im * lam_im
    inv_re = diag_re / denom
    inv_im = -lam_im / denom
    sol_re = spec_re * inv_re - spec_im * inv_im
    sol_im = spec_re * inv_im + spec_im * inv_re
    for sweep in range(SWEEPS - 1):
        stiff_re, stiff_im = stiffness_pair(sol_re, sol_im, diffusivity)
        sol_re, sol_im = jacobi_step(
            spec_re, spec_im, sol_re, sol_im, stiff_re, stiff_im, lam_re, lam_im, inv_re, inv_im
        )
    stiff_re, stiff_im = stiffness_pair(sol_re, sol_im, diffusivity)
    sol_re, sol_im, stiff_re, stiff_im = (
        lax.all_to_all(
            sol_re.reshape(steps_here, cells), "tm", split_axis=1, concat_axis=0, tiled=True
        ),
        lax.all_to_all(
            sol_im.reshape(steps_here, cells), "tm", split_axis=1, concat_axis=0, tiled=True
        ),
        lax.all_to_all(
            stiff_re.reshape(steps_here, cells), "tm", split_axis=1, concat_axis=0, tiled=True
        ),
        lax.all_to_all(
            stiff_im.reshape(steps_here, cells), "tm", split_axis=1, concat_axis=0, tiled=True
        ),
    )
    correction = (time_product(cos_table, sol_re) - time_product(sin_table, sol_im)) / total
    stiff_time = (time_product(cos_table, stiff_re) - time_product(sin_table, stiff_im)) / total
    image = time_product(toeplitz, correction) + stiff_time
    inner_ri, inner_ii = inner_products(residual, image)
    step = inner_ri / inner_ii
    new_residual = residual - step * image
    correction_slab, residual_back = (
        lax.all_to_all(correction, "tm", split_axis=0, concat_axis=1, tiled=True),
        lax.all_to_all(new_residual, "tm", split_axis=0, concat_axis=1, tiled=True),
    )
    new_iterate = iterate + step * correction_slab.reshape(slab_shape)
    return (new_iterate, residual_back.reshape(slab_shape))


def constants(total):
    scale = 1.0 / (step_length**frac_order * gamma_factor)
    power = 1.0 - frac_order
    b = [(k + 1.0) ** power - float(k) ** power for k in range(total)]
    d = [scale * (b[k] - (b[k - 1] if k else 0.0)) for k in range(total)]
    angle = [2.0 * math.pi * i / total for i in range(total)]
    cos = [math.cos(a) for a in angle]
    sin = [math.sin(a) for a in angle]
    half = total // 2
    lam_re = [sum(d[k] * cos[j * k % total] for k in range(half)) for j in range(total)]
    lam_im = [-sum(d[k] * sin[j * k % total] for k in range(half)) for j in range(total)]
    return d, cos, sin, lam_re, lam_im


def weighted(terms):
    result = None
    for weight, value in terms:
        if abs(weight) < 1e-9:
            continue
        if result is None:
            result = value if abs(weight - 1.0) < 1e-9 else weight * value
        elif abs(weight - 1.0) < 1e-9:
            result = result + value
        elif abs(weight + 1.0) < 1e-9:
            result = result - value
        else:
            result = result + weight * value
    return result


def pick(index, values):
    result = jnp.float32(values[0])
    for i in range(1, len(values)):
        result = jnp.where(index == i, jnp.float32(values[i]), result)
    return result


def fused_kernel(
    peers,
    u_hbm,
    f_hbm,
    k_hbm,
    x_out,
    r_out,
    u,
    f,
    kap,
    kap_far,
    u_halo,
    wbuf,
    got_uw,
    res,
    spec,
    got_spec,
    far_spec,
    got_res,
    gain,
    hop,
    sol_0,
    sol_a,
    sol_b,
    xy,
    got_xy,
    ci,
    got_ci,
    part,
    got_part,
    load_sem,
    halo_send,
    halo_recv,
    kap_send,
    kap_recv,
    uw_send,
    uw_recv,
    spec_send,
    spec_recv,
    far_send,
    far_recv,
    res_send,
    res_recv,
    xy_send,
    xy_recv,
    ci_send,
    ci_recv,
    part_send,
    part_recv,
):
    me = lax.axis_index("tm")
    side = lax.axis_index("space")
    ny, nx = u.shape[-2:]
    reach = SWEEPS
    low = peers - reach
    d, cos, sin, lam_re, lam_im = constants(peers)
    half = peers // 2
    others = [lax.rem(me + i, peers) for i in range(1, peers)]
    mesh_type = pl.DeviceIdType.MESH

    def plane(q):
        return side * (peers - 1) + q * (1 - 2 * side)

    def at_tm(k):
        return {"tm": k}

    across = {"space": 1 - side}

    def diagonal(k):
        return {"tm": k, "space": 1 - side}

    def copy(src, dst, send, recv, device):
        return pltpu.make_async_remote_copy(
            src_ref=src,
            dst_ref=dst,
            send_sem=send,
            recv_sem=recv,
            device_id=device,
            device_id_type=mesh_type,
        )

    loads = [
        pltpu.make_async_copy(a, b, load_sem.at[i])
        for i, (a, b) in enumerate(((u_hbm.at[0], u), (k_hbm, kap), (f_hbm.at[0], f)))
    ]
    for load in loads:
        load.start()
    barrier = pltpu.get_barrier_semaphore()
    for k in others:
        pl.semaphore_signal(barrier, inc=1, device_id=at_tm(k), device_id_type=mesh_type)
        pl.semaphore_signal(barrier, inc=1, device_id=diagonal(k), device_id_type=mesh_type)
    pl.semaphore_signal(barrier, inc=1, device_id=across, device_id_type=mesh_type)
    loads[0].wait()
    loads[1].wait()
    loads[2].wait()

    rows = lax.broadcasted_iota(jnp.int32, (ny, nx), 0)
    lanes = lax.broadcasted_iota(jnp.int32, (ny, nx), 1)
    not_top = rows > 0
    not_bottom = rows < ny - 1
    not_left = lanes > 0
    not_right = lanes < nx - 1

    def in_plane(v):
        y = jnp.where(not_top, pltpu.roll(v, 1, 0), 0.0) + jnp.where(
            not_bottom, pltpu.roll(v, ny - 1, 0), 0.0
        )
        x = jnp.where(not_left, pltpu.roll(v, 1, 1), 0.0) + jnp.where(
            not_right, pltpu.roll(v, nx - 1, 1), 0.0
        )
        return y + x

    pl.semaphore_wait(barrier, 2 * peers - 1)
    halo = copy(u.at[plane(peers - 1)], u_halo, halo_send, halo_recv, across)
    halo.start()
    sends = [halo]
    for k in others:
        c = copy(
            u.at[plane(k)], got_uw.at[me, 0], uw_send.at[k, 0], uw_recv.at[me, 0], at_tm(k)
        )
        c.start()
        sends.append(c)
    kap_copy = copy(kap, kap_far, kap_send, kap_recv, across)
    kap_copy.start()
    sends.append(kap_copy)

    def stiff_of_iterate(q, after):
        value = u[plane(q)]
        total = in_plane(value) + after
        if q > 0:
            total = total + u[plane(q - 1)]
        wbuf[q] = f[plane(q)] - kap[plane(q)] * (6.0 * value - total)

    for q in range(peers - 1):
        stiff_of_iterate(q, u[plane(q + 1)])
    halo.wait_recv()
    stiff_of_iterate(peers - 1, u_halo[...])
    for k in others:
        c = copy(wbuf.at[k], got_uw.at[me, 1], uw_send.at[k, 1], uw_recv.at[me, 1], at_tm(k))
        c.start()
        sends.append(c)
    got_uw[me, 0] = u[plane(me)]
    got_uw[me, 1] = wbuf[me]

    my_re = pick(me, lam_re)
    my_im = pick(me, lam_im)
    kap_copy.wait_recv()
    depth = peers + reach
    for q in range(depth):
        kappa = kap[plane(q)] if q < peers else kap_far[(1 - side) * (peers - 1) + (2 * peers - 1 - q) * (2 * side - 1)]
        diag = my_re + 6.0 * kappa
        inverse = 1.0 / (diag * diag + my_im * my_im)
        g_re = diag * inverse
        g_im = -my_im * inverse
        gain[q, 0] = g_re
        gain[q, 1] = g_im
        hop[q, 0] = g_re * kappa
        hop[q, 1] = g_im * kappa
    zero = jnp.zeros((ny, nx), jnp.float32)
    for buffer in (sol_0, sol_a, sol_b):
        buffer[0, 0] = zero
        buffer[0, 1] = zero

    for k in others:
        for i in range(2):
            copy(
                wbuf.at[k], got_uw.at[k, i], uw_send.at[k, i], uw_recv.at[k, i], at_tm(k)
            ).wait_recv()
    residual = []
    for n in range(peers):
        history = weighted([(d[n - m], got_uw[m, 0]) for m in range(n + 1)])
        value = got_uw[n, 1] - history
        res[n] = value
        residual.append(value)
    for j in range(half + 1):
        real = weighted([(cos[j * n % peers], residual[n]) for n in range(peers)])
        imag = weighted([(-sin[j * n % peers], residual[n]) for n in range(peers)])
        if imag is None:
            imag = zero
        spec[j, 0] = real
        spec[j, 1] = imag
        if 0 < j < half:
            spec[peers - j, 0] = real
            spec[peers - j, 1] = -imag
    for k in others:
        c = copy(spec.at[k], got_spec.at[me], spec_send.at[k], spec_recv.at[me], at_tm(k))
        c.start()
        sends.append(c)
    got_spec[me] = spec[me]

    def forward(q):
        return copy(got_spec.at[q], far_spec.at[q], far_send.at[q], far_recv.at[q], across)

    @pl.when(me >= low)
    def _():
        copy(spec.at[me], far_spec.at[me], far_send.at[me], far_recv.at[me], across).start()

    for k in others:
        copy(spec.at[k], got_spec.at[k], spec_send.at[k], spec_recv.at[k], at_tm(k)).wait_recv()

        @pl.when(k >= low)
        def _():
            forward(k).start()

    for k in others:
        c = copy(res.at[k], got_res.at[me], res_send.at[k], res_recv.at[me], at_tm(k))
        c.start()
        sends.append(c)
    got_res[me] = res[me]

    def first_solution(q, s):
        g_re, g_im = gain[q, 0], gain[q, 1]
        s_re, s_im = s[0], s[1]
        sol_0[q + 1, 0] = s_re * g_re - s_im * g_im
        sol_0[q + 1, 1] = s_re * g_im + s_im * g_re

    for q in range(peers):
        first_solution(q, got_spec[q])
    for q in range(low, peers):
        forward(q).wait_recv()
    for q in range(peers, depth):
        first_solution(q, far_spec[2 * peers - 1 - q])

    def neighbours(buffer, q, i):
        return buffer[q, i] + buffer[q + 2, i] + in_plane(buffer[q + 1, i])

    now = sol_0
    for sweep in range(SWEEPS - 1):
        later = sol_b if now is sol_a else sol_a

        def sweep_plane(q, carry, now=now, later=later):
            n_re = neighbours(now, q, 0)
            n_im = neighbours(now, q, 1)
            h_re, h_im = hop[q, 0], hop[q, 1]
            later[q + 1, 0] = sol_0[q + 1, 0] + (h_re * n_re - h_im * n_im)
            later[q + 1, 1] = sol_0[q + 1, 1] + (h_re * n_im + h_im * n_re)
            return carry

        lax.fori_loop(0, depth - 1 - sweep, sweep_plane, 0, unroll=True)
        now = later

    is_sol = me <= half
    is_real = jnp.logical_or(me == 0, me == half)

    def stiff_plane(q, carry):
        kappa = kap[plane(q)]
        s_re, s_im = now[q + 1, 0], now[q + 1, 1]
        k_re = kappa * (6.0 * s_re - neighbours(now, q, 0))
        k_im = kappa * (6.0 * s_im - neighbours(now, q, 1))
        xy[q, 0] = jnp.where(is_sol, s_re, k_re)
        xy[q, 1] = jnp.where(is_real, k_re, jnp.where(is_sol, s_im, k_im))
        return carry

    lax.fori_loop(0, peers, stiff_plane, 0, unroll=True)
    for k in others:
        c = copy(xy.at[k], got_xy.at[me], xy_send.at[k], xy_recv.at[me], at_tm(k))
        c.start()
        sends.append(c)
    got_xy[me] = xy[me]
    for k in others:
        copy(xy.at[k], got_xy.at[k], xy_send.at[k], xy_recv.at[k], at_tm(k)).wait_recv()

    inv = 1.0 / peers
    corrections = []
    for n in range(peers):
        terms = [(inv, got_xy[0, 0]), (inv * cos[n * half % peers], got_xy[half, 0])]
        for j in range(1, half):
            terms.append((2.0 * inv * cos[n * j % peers], got_xy[j, 0]))
            terms.append((-2.0 * inv * sin[n * j % peers], got_xy[j, 1]))
        value = weighted(terms)
        ci[n, 0] = value
        corrections.append(value)
    inner_ri = zero
    inner_ii = zero
    for n in range(peers):
        terms = [(inv, got_xy[0, 1]), (inv * cos[n * half % peers], got_xy[half, 1])]
        for j in range(half + 1, peers):
            terms.append((2.0 * inv * cos[n * j % peers], got_xy[j, 0]))
            terms.append((-2.0 * inv * sin[n * j % peers], got_xy[j, 1]))
        image = weighted(terms + [(d[n - m], corrections[m]) for m in range(n + 1)])
        ci[n, 1] = image
        inner_ri = inner_ri + res[n] * image
        inner_ii = inner_ii + image * image
    part[0:1] = jnp.sum(inner_ri, axis=0, keepdims=True)
    part[1:2] = jnp.sum(inner_ii, axis=0, keepdims=True)
    mine = side * peers + me
    opposite = (1 - side) * peers

    def part_copy(slot, source, device):
        return copy(part, got_part.at[source], part_send.at[slot], part_recv.at[source], device)

    for k in others:
        for slot, device in ((side * peers + k, at_tm(k)), (opposite + k, diagonal(k))):
            c = part_copy(slot, mine, device)
            c.start()
            sends.append(c)
    c = part_copy(opposite + me, mine, across)
    c.start()
    sends.append(c)
    for k in others:
        c = copy(ci.at[k], got_ci.at[me], ci_send.at[k], ci_recv.at[me], at_tm(k))
        c.start()
        sends.append(c)
    got_ci[me] = ci[me]
    got_part[mine] = part[...]
    for k in others:
        copy(res.at[k], got_res.at[k], res_send.at[k], res_recv.at[k], at_tm(k)).wait_recv()
    for k in others:
        part_copy(side * peers + k, side * peers + k, at_tm(k)).wait_recv()
        part_copy(opposite + k, opposite + k, diagonal(k)).wait_recv()
    part_copy(opposite + me, opposite + me, across).wait_recv()
    sums = got_part[0]
    for i in range(1, 2 * peers):
        sums = sums + got_part[i]
    sums = jnp.sum(sums, axis=1, keepdims=True)
    step = sums[0:1] / sums[1:2]
    for k in others:
        copy(ci.at[k], got_ci.at[k], ci_send.at[k], ci_recv.at[k], at_tm(k)).wait_recv()
    for q in range(peers):
        x_out[0, plane(q)] = u[plane(q)] + step * got_ci[q, 0]
        r_out[0, plane(q)] = got_res[q] - step * got_ci[q, 1]
    for c in sends:
        c.wait_send()
    for q in range(low, peers):
        forward(q).wait_send()


def fused(iterate, source, diffusivity):
    peers = lax.axis_size("tm")
    ny, nx = iterate.shape[-2:]
    depth = peers + SWEEPS

    def buffer(*lead):
        return pltpu.VMEM(lead + (ny, nx), jnp.float32)

    dma = pltpu.SemaphoreType.DMA
    shape = jax.ShapeDtypeStruct(iterate.shape, jnp.float32)
    vmem = pl.BlockSpec(memory_space=pltpu.VMEM)
    return pl.pallas_call(
        functools.partial(fused_kernel, peers),
        out_shape=(shape, shape),
        in_specs=[pl.BlockSpec(memory_space=pl.ANY)] * 3,
        out_specs=(vmem, vmem),
        scratch_shapes=[
            buffer(peers),
            buffer(peers),
            buffer(peers),
            buffer(peers),
            buffer(),
            buffer(peers),
            buffer(peers, 2),
            buffer(peers),
            buffer(peers, 2),
            buffer(peers, 2),
            buffer(peers, 2),
            buffer(peers),
            buffer(depth, 2),
            buffer(depth, 2),
            buffer(depth + 1, 2),
            buffer(depth + 1, 2),
            buffer(depth + 1, 2),
            buffer(peers, 2),
            buffer(peers, 2),
            buffer(peers, 2),
            buffer(peers, 2),
            pltpu.VMEM((2, nx), jnp.float32),
            pltpu.VMEM((2 * peers, 2, nx), jnp.float32),
            dma((3,)),
            dma,
            dma,
            dma,
            dma,
            dma((peers, 2)),
            dma((peers, 2)),
            dma((peers,)),
            dma((peers,)),
            dma((peers,)),
            dma((peers,)),
            dma((peers,)),
            dma((peers,)),
            dma((peers,)),
            dma((peers,)),
            dma((peers,)),
            dma((peers,)),
            dma((2 * peers,)),
            dma((2 * peers,)),
        ],
        compiler_params=pltpu.CompilerParams(collective_id=0, has_side_effects=True),
    )(iterate, source, diffusivity)


def on_device_any(iterate, source, diffusivity):
    steps, planes, ny, nx = iterate.shape
    peers = lax.axis_size("tm")
    fits = (
        steps == 1
        and planes == peers
        and peers % 2 == 0
        and lax.axis_size("space") == 2
        and planes >= SWEEPS
        and ny % 8 == 0
        and nx % 128 == 0
    )
    return (fused if fits else on_device)(iterate, source, diffusivity)


def solution(mesh):
    in_specs = (
        P(("groups", "tm"), "space", None, None),
        P(("groups", "tm"), "space", None, None),
        P(("groups", "space"), None, None),
    )
    out_specs = (P(("groups", "tm"), "space", None, None), P(("groups", "tm"), "space", None, None))
    return jax.shard_map(
        on_device_any, mesh=mesh, in_specs=in_specs, out_specs=out_specs, check_vma=False
    )
```

```python
import functools
import math

import jax
import jax.numpy as jnp
from jax import lax
from jax.experimental import pallas as pl
from jax.experimental.pallas import tpu as pltpu
from jax.sharding import PartitionSpec as P

SWEEPS = 6


frac_order = 0.3
step_length = 0.01
gamma_factor = 0.9086387328532904


def with_halo(value, sides, width):
    for axis, dim in sides:
        peers, length = (lax.axis_size(axis), value.shape[dim])
        up = [(i, (i + 1) % peers) for i in range(peers - 1)]
        down = [(j, i) for i, j in up]
        last = lax.slice_in_dim(value, length - width, length, axis=dim)
        first = lax.slice_in_dim(value, 0, width, axis=dim)
        before = lax.ppermute(last, axis, up)
        after = lax.ppermute(first, axis, down)
        value = jnp.concatenate([before, value, after], axis=dim)
    return value


def history_weights(lags):
    scale = 1.0 / (step_length**frac_order * gamma_factor)
    power = 1.0 - frac_order
    safe = jnp.maximum(lags, 0.0)
    upper = (safe + 1.0) ** power - safe**power
    lower = jnp.where(safe >= 1.0, safe**power - jnp.maximum(safe - 1.0, 0.0) ** power, 0.0)
    return jnp.where(lags >= 0.0, (upper - lower) * scale, 0.0)


def circulant_spectrum(freqs, total):
    lags = jnp.arange(total, dtype=jnp.int32)
    first = jnp.where(lags < total // 2, history_weights(lags.astype(jnp.float32)), 0.0)
    phase = (freqs[:, None] * lags[None, :] % total).astype(jnp.float32) * (2.0 * math.pi / total)
    real_part = jnp.sum(first[None, :] * jnp.cos(phase), axis=1)
    imag_part = -jnp.sum(first[None, :] * jnp.sin(phase), axis=1)
    return (real_part, imag_part)


def fourier_tables(total):
    index = jnp.arange(total, dtype=jnp.int32)
    phase = (index[:, None] * index[None, :] % total).astype(jnp.float32) * (2.0 * math.pi / total)
    return (jnp.cos(phase), jnp.sin(phase))


def neighbour_sum(padded):
    inner = padded[..., 1:-1, :, :]
    result = padded[..., 2:, :, :] + padded[..., :-2, :, :]
    along_y = jnp.pad(inner, [(0, 0)] * (inner.ndim - 2) + [(1, 1), (0, 0)])
    result = result + along_y[..., 2:, :] + along_y[..., :-2, :]
    along_x = jnp.pad(inner, [(0, 0)] * (inner.ndim - 1) + [(1, 1)])
    return result + along_x[..., 2:] + along_x[..., :-2]


def jacobi_step(
    spec_re, spec_im, sol_re, sol_im, stiff_re, stiff_im, lam_re, lam_im, inv_re, inv_im
):
    res_re = spec_re - (lam_re * sol_re - lam_im * sol_im) - stiff_re
    res_im = spec_im - (lam_re * sol_im + lam_im * sol_re) - stiff_im
    return (
        sol_re + (res_re * inv_re - res_im * inv_im),
        sol_im + (res_re * inv_im + res_im * inv_re),
    )


def stiffness_pair(sol_re, sol_im, diffusivity):
    stacked = jnp.stack([sol_re, sol_im])
    padded = with_halo(stacked, (("space", 2),), 1)
    stiff = diffusivity * (6.0 * stacked - neighbour_sum(padded))
    return (stiff[0], stiff[1])


def time_product(matrix, field):
    return jnp.dot(matrix, field, precision=lax.Precision.HIGHEST)


def inner_products(residual, image):
    return lax.psum((jnp.sum(residual * image), jnp.sum(image * image)), ("tm", "space"))


def on_device(iterate, source, diffusivity):
    steps_here = iterate.shape[0]
    slab_shape = iterate.shape
    cells = slab_shape[1] * slab_shape[2] * slab_shape[3]
    total = steps_here * lax.axis_size("tm")
    my_times = lax.axis_index("tm") * steps_here + jnp.arange(steps_here, dtype=jnp.int32)
    times = jnp.arange(total, dtype=jnp.int32)
    toeplitz = history_weights((times[:, None] - times[None, :]).astype(jnp.float32))
    cos_table, sin_table = fourier_tables(total)
    padded = with_halo(iterate, (("space", 1),), 1)
    stiff_iter = diffusivity * (6.0 * iterate - neighbour_sum(padded))
    flat_iter = iterate.reshape(steps_here, cells)
    flat_source = source.reshape(steps_here, cells)
    flat_stiff = stiff_iter.reshape(steps_here, cells)
    iter_cols, source_cols, stiff_cols = (
        lax.all_to_all(flat_iter, "tm", split_axis=1, concat_axis=0, tiled=True),
        lax.all_to_all(flat_source, "tm", split_axis=1, concat_axis=0, tiled=True),
        lax.all_to_all(flat_stiff, "tm", split_axis=1, concat_axis=0, tiled=True),
    )
    residual = source_cols - time_product(toeplitz, iter_cols) - stiff_cols
    spec_re = time_product(cos_table, residual)
    spec_im = -time_product(sin_table, residual)
    spec_re, spec_im = (
        lax.all_to_all(spec_re, "tm", split_axis=0, concat_axis=1, tiled=True),
        lax.all_to_all(spec_im, "tm", split_axis=0, concat_axis=1, tiled=True),
    )
    spec_re = spec_re.reshape(slab_shape)
    spec_im = spec_im.reshape(slab_shape)
    lam_re, lam_im = circulant_spectrum(my_times, total)
    lam_re = lam_re[:, None, None, None]
    lam_im = lam_im[:, None, None, None]
    diag_re = lam_re + 6.0 * diffusivity
    denom = diag_re * diag_re + lam_im * lam_im
    inv_re = diag_re / denom
    inv_im = -lam_im / denom
    sol_re = spec_re * inv_re - spec_im * inv_im
    sol_im = spec_re * inv_im + spec_im * inv_re
    for sweep in range(SWEEPS - 1):
        stiff_re, stiff_im = stiffness_pair(sol_re, sol_im, diffusivity)
        sol_re, sol_im = jacobi_step(
            spec_re, spec_im, sol_re, sol_im, stiff_re, stiff_im, lam_re, lam_im, inv_re, inv_im
        )
    stiff_re, stiff_im = stiffness_pair(sol_re, sol_im, diffusivity)
    sol_re, sol_im, stiff_re, stiff_im = (
        lax.all_to_all(
            sol_re.reshape(steps_here, cells), "tm", split_axis=1, concat_axis=0, tiled=True
        ),
        lax.all_to_all(
            sol_im.reshape(steps_here, cells), "tm", split_axis=1, concat_axis=0, tiled=True
        ),
        lax.all_to_all(
            stiff_re.reshape(steps_here, cells), "tm", split_axis=1, concat_axis=0, tiled=True
        ),
        lax.all_to_all(
            stiff_im.reshape(steps_here, cells), "tm", split_axis=1, concat_axis=0, tiled=True
        ),
    )
    correction = (time_product(cos_table, sol_re) - time_product(sin_table, sol_im)) / total
    stiff_time = (time_product(cos_table, stiff_re) - time_product(sin_table, stiff_im)) / total
    image = time_product(toeplitz, correction) + stiff_time
    inner_ri, inner_ii = inner_products(residual, image)
    step = inner_ri / inner_ii
    new_residual = residual - step * image
    correction_slab, residual_back = (
        lax.all_to_all(correction, "tm", split_axis=0, concat_axis=1, tiled=True),
        lax.all_to_all(new_residual, "tm", split_axis=0, concat_axis=1, tiled=True),
    )
    new_iterate = iterate + step * correction_slab.reshape(slab_shape)
    return (new_iterate, residual_back.reshape(slab_shape))


def constants(total):
    scale = 1.0 / (step_length**frac_order * gamma_factor)
    power = 1.0 - frac_order
    b = [(k + 1.0) ** power - float(k) ** power for k in range(total)]
    d = [scale * (b[k] - (b[k - 1] if k else 0.0)) for k in range(total)]
    angle = [2.0 * math.pi * i / total for i in range(total)]
    cos = [math.cos(a) for a in angle]
    sin = [math.sin(a) for a in angle]
    half = total // 2
    lam_re = [sum(d[k] * cos[j * k % total] for k in range(half)) for j in range(total)]
    lam_im = [-sum(d[k] * sin[j * k % total] for k in range(half)) for j in range(total)]
    return d, cos, sin, lam_re, lam_im


def weighted(terms):
    result = None
    for weight, value in terms:
        if abs(weight) < 1e-9:
            continue
        if result is None:
            result = value if abs(weight - 1.0) < 1e-9 else weight * value
        elif abs(weight - 1.0) < 1e-9:
            result = result + value
        elif abs(weight + 1.0) < 1e-9:
            result = result - value
        else:
            result = result + weight * value
    return result


def pick(index, values):
    result = jnp.float32(values[0])
    for i in range(1, len(values)):
        result = jnp.where(index == i, jnp.float32(values[i]), result)
    return result


def exchange_order(me, peers):
    if peers & (peers - 1):
        return [lax.rem(me + i, peers) for i in range(1, peers)]
    bits = range(peers.bit_length() - 1)
    result = []
    for mask in range(peers - 1, 0, -1):
        partner = 0
        for b in bits:
            digit = lax.rem(me // (1 << b), 2)
            partner = partner + ((1 - digit) if mask >> b & 1 else digit) * (1 << b)
        result.append(partner)
    return result


def fused_kernel(
    peers,
    u_hbm,
    f_hbm,
    k_hbm,
    x_out,
    r_out,
    dr_out,
    u,
    f,
    kap,
    kap_far,
    u_halo,
    wbuf,
    got_uw,
    res,
    spec,
    got_spec,
    far_spec,
    got_res,
    gain,
    hop,
    sols,
    xy,
    got_xy,
    ci,
    got_ci,
    part,
    got_part,
    load_sem,
    halo_send,
    halo_recv,
    kap_send,
    kap_recv,
    uw_send,
    uw_recv,
    spec_send,
    spec_recv,
    far_send,
    far_recv,
    res_send,
    res_recv,
    xy_send,
    xy_recv,
    ci_send,
    ci_recv,
    part_send,
    part_recv,
):
    me = lax.axis_index("tm")
    side = lax.axis_index("space")
    ny, nx = u.shape[-2:]
    reach = SWEEPS
    low = peers - reach
    d, cos, sin, lam_re, lam_im = constants(peers)
    half = peers // 2
    others = exchange_order(me, peers)
    mesh_type = pl.DeviceIdType.MESH

    def plane(q):
        return side * (peers - 1) + q * (1 - 2 * side)

    def at_tm(k):
        return {"tm": k}

    across = {"space": 1 - side}

    def diagonal(k):
        return {"tm": k, "space": 1 - side}

    def copy(src, dst, send, recv, device):
        return pltpu.make_async_remote_copy(
            src_ref=src,
            dst_ref=dst,
            send_sem=send,
            recv_sem=recv,
            device_id=device,
            device_id_type=mesh_type,
        )

    loads = [
        pltpu.make_async_copy(a, b, load_sem.at[i])
        for i, (a, b) in enumerate(((u_hbm.at[0], u), (k_hbm, kap), (f_hbm.at[0], f)))
    ]
    for load in loads:
        load.start()
    barrier = pltpu.get_barrier_semaphore()
    for k in others:
        pl.semaphore_signal(barrier, inc=1, device_id=at_tm(k), device_id_type=mesh_type)
    pl.semaphore_signal(barrier, inc=1, device_id=across, device_id_type=mesh_type)
    loads[0].wait()
    loads[1].wait()
    loads[2].wait()

    rows = lax.broadcasted_iota(jnp.int32, (ny, nx), 0)
    lanes = lax.broadcasted_iota(jnp.int32, (ny, nx), 1)
    not_top = rows > 0
    not_bottom = rows < ny - 1
    not_left = lanes > 0
    not_right = lanes < nx - 1

    def in_plane(v):
        y = jnp.where(not_top, pltpu.roll(v, 1, 0), 0.0) + jnp.where(
            not_bottom, pltpu.roll(v, ny - 1, 0), 0.0
        )
        x = jnp.where(not_left, pltpu.roll(v, 1, 1), 0.0) + jnp.where(
            not_right, pltpu.roll(v, nx - 1, 1), 0.0
        )
        return y + x

    pl.semaphore_wait(barrier, peers)
    halo = copy(u.at[plane(peers - 1)], u_halo, halo_send, halo_recv, across)
    halo.start()
    sends = [halo]
    for k in others:
        c = copy(
            u.at[plane(k)], got_uw.at[me, 0], uw_send.at[k, 0], uw_recv.at[me, 0], at_tm(k)
        )
        c.start()
        sends.append(c)
    kap_copy = copy(kap, kap_far, kap_send, kap_recv, across)
    kap_copy.start()
    sends.append(kap_copy)

    def stiff_of_iterate(q, after):
        value = u[plane(q)]
        total = in_plane(value) + after
        if q > 0:
            total = total + u[plane(q - 1)]
        wbuf[q] = f[plane(q)] - kap[plane(q)] * (6.0 * value - total)

    for q in range(peers - 1):
        stiff_of_iterate(q, u[plane(q + 1)])
    halo.wait_recv()
    stiff_of_iterate(peers - 1, u_halo[...])
    for k in others:
        c = copy(wbuf.at[k], got_uw.at[me, 1], uw_send.at[k, 1], uw_recv.at[me, 1], at_tm(k))
        c.start()
        sends.append(c)
    got_uw[me, 0] = u[plane(me)]
    got_uw[me, 1] = wbuf[me]

    my_re = pick(me, lam_re)
    my_im = pick(me, lam_im)
    kap_copy.wait_recv()
    depth = peers + reach
    for q in range(depth):
        kappa = kap[plane(q)] if q < peers else kap_far[(1 - side) * (peers - 1) + (2 * peers - 1 - q) * (2 * side - 1)]
        diag = my_re + 6.0 * kappa
        inverse = 1.0 / (diag * diag + my_im * my_im)
        g_re = diag * inverse
        g_im = -my_im * inverse
        gain[q, 0] = g_re
        gain[q, 1] = g_im
        hop[q, 0] = g_re * kappa
        hop[q, 1] = g_im * kappa
    zero = jnp.zeros((ny, nx), jnp.float32)
    for level in range(SWEEPS):
        sols[level, 0, 0] = zero
        sols[level, 0, 1] = zero

    for k in others:
        for i in range(2):
            copy(
                wbuf.at[k], got_uw.at[k, i], uw_send.at[k, i], uw_recv.at[k, i], at_tm(k)
            ).wait_recv()
    residual = []
    for n in range(peers):
        history = weighted([(d[n - m], got_uw[m, 0]) for m in range(n + 1)])
        value = got_uw[n, 1] - history
        res[n] = value
        residual.append(value)
    for j in range(half + 1):
        real = weighted([(cos[j * n % peers], residual[n]) for n in range(peers)])
        imag = weighted([(-sin[j * n % peers], residual[n]) for n in range(peers)])
        if imag is None:
            imag = zero
        spec[j, 0] = real
        spec[j, 1] = imag
        if 0 < j < half:
            spec[peers - j, 0] = real
            spec[peers - j, 1] = -imag
    for k in others:
        c = copy(spec.at[k], got_spec.at[me], spec_send.at[k], spec_recv.at[me], at_tm(k))
        c.start()
        sends.append(c)
    got_spec[me] = spec[me]

    def forward(q):
        return copy(got_spec.at[q], far_spec.at[q], far_send.at[q], far_recv.at[q], across)

    @pl.when(me >= low)
    def _():
        copy(spec.at[me], far_spec.at[me], far_send.at[me], far_recv.at[me], across).start()

    for k in others:
        copy(spec.at[k], got_spec.at[k], spec_send.at[k], spec_recv.at[k], at_tm(k)).wait_recv()

        @pl.when(k >= low)
        def _():
            forward(k).start()

    for k in others:
        c = copy(res.at[k], got_res.at[me], res_send.at[k], res_recv.at[me], at_tm(k))
        c.start()
        sends.append(c)
    got_res[me] = res[me]

    def first_solution(q, s):
        g_re, g_im = gain[q, 0], gain[q, 1]
        s_re, s_im = s[0], s[1]
        sols[0, q + 1, 0] = s_re * g_re - s_im * g_im
        sols[0, q + 1, 1] = s_re * g_im + s_im * g_re

    def neighbours(buffer, q, i):
        return buffer[q, i] + buffer[q + 2, i] + in_plane(buffer[q + 1, i])

    def sweep_plane(level, q):
        before = sols.at[level - 1]
        n_re = neighbours(before, q, 0)
        n_im = neighbours(before, q, 1)
        h_re, h_im = hop[q, 0], hop[q, 1]
        sols[level, q + 1, 0] = sols[0, q + 1, 0] + (h_re * n_re - h_im * n_im)
        sols[level, q + 1, 1] = sols[0, q + 1, 1] + (h_re * n_im + h_im * n_re)

    for q in range(peers):
        first_solution(q, got_spec[q])
    for level in range(1, SWEEPS):
        lax.fori_loop(0, peers - level, lambda q, c, level=level: sweep_plane(level, q), None, unroll=True)
    for q in range(low, peers):
        forward(q).wait_recv()
    for q in range(peers, depth):
        first_solution(q, far_spec[2 * peers - 1 - q])
    for level in range(1, SWEEPS):
        lax.fori_loop(
            peers - level,
            depth - level,
            lambda q, c, level=level: sweep_plane(level, q),
            None,
            unroll=True,
        )
    now = sols.at[SWEEPS - 1]

    is_sol = me <= half
    is_real = jnp.logical_or(me == 0, me == half)

    def stiff_plane(q, carry):
        kappa = kap[plane(q)]
        s_re, s_im = now[q + 1, 0], now[q + 1, 1]
        k_re = kappa * (6.0 * s_re - neighbours(now, q, 0))
        k_im = kappa * (6.0 * s_im - neighbours(now, q, 1))
        xy[q, 0] = jnp.where(is_sol, s_re, k_re)
        xy[q, 1] = jnp.where(is_real, k_re, jnp.where(is_sol, s_im, k_im))
        return carry

    lax.fori_loop(0, peers, stiff_plane, 0, unroll=True)
    for k in others:
        c = copy(xy.at[k], got_xy.at[me], xy_send.at[k], xy_recv.at[me], at_tm(k))
        c.start()
        sends.append(c)
    got_xy[me] = xy[me]
    for k in others:
        copy(xy.at[k], got_xy.at[k], xy_send.at[k], xy_recv.at[k], at_tm(k)).wait_recv()

    inv = 1.0 / peers
    corrections = []
    for n in range(peers):
        terms = [(inv, got_xy[0, 0]), (inv * cos[n * half % peers], got_xy[half, 0])]
        for j in range(1, half):
            terms.append((2.0 * inv * cos[n * j % peers], got_xy[j, 0]))
            terms.append((-2.0 * inv * sin[n * j % peers], got_xy[j, 1]))
        value = weighted(terms)
        ci[n, 0] = value
        corrections.append(value)
    inner_ri = zero
    inner_ii = zero
    for n in range(peers):
        terms = [(inv, got_xy[0, 1]), (inv * cos[n * half % peers], got_xy[half, 1])]
        for j in range(half + 1, peers):
            terms.append((2.0 * inv * cos[n * j % peers], got_xy[j, 0]))
            terms.append((-2.0 * inv * sin[n * j % peers], got_xy[j, 1]))
        image = weighted(terms + [(d[n - m], corrections[m]) for m in range(n + 1)])
        ci[n, 1] = image
        inner_ri = inner_ri + res[n] * image
        inner_ii = inner_ii + image * image
    part[0:1] = jnp.sum(inner_ri, axis=0, keepdims=True)
    part[1:2] = jnp.sum(inner_ii, axis=0, keepdims=True)
    mine = side * peers + me
    opposite = (1 - side) * peers

    def part_copy(slot, source, device):
        return copy(part, got_part.at[source], part_send.at[slot], part_recv.at[source], device)

    for k in others:
        for slot, device in ((side * peers + k, at_tm(k)), (opposite + k, diagonal(k))):
            c = part_copy(slot, mine, device)
            c.start()
            sends.append(c)
    c = part_copy(opposite + me, mine, across)
    c.start()
    sends.append(c)
    for k in others:
        c = copy(ci.at[k], got_ci.at[me], ci_send.at[k], ci_recv.at[me], at_tm(k))
        c.start()
        sends.append(c)
    got_ci[me] = ci[me]
    got_part[mine] = part[...]
    for k in others:
        copy(res.at[k], got_res.at[k], res_send.at[k], res_recv.at[k], at_tm(k)).wait_recv()
    for q in range(peers):
        r_out[0, plane(q)] = got_res[q]
    for k in others:
        part_copy(side * peers + k, side * peers + k, at_tm(k)).wait_recv()
        part_copy(opposite + k, opposite + k, diagonal(k)).wait_recv()
    part_copy(opposite + me, opposite + me, across).wait_recv()
    sums = got_part[0]
    for i in range(1, 2 * peers):
        sums = sums + got_part[i]
    sums = jnp.sum(sums, axis=1, keepdims=True)
    step = sums[0:1] / sums[1:2]
    for k in others:
        copy(ci.at[k], got_ci.at[k], ci_send.at[k], ci_recv.at[k], at_tm(k)).wait_recv()
    for q in range(peers):
        x_out[0, plane(q)] = step * got_ci[q, 0]
        dr_out[0, plane(q)] = step * got_ci[q, 1]
    for c in sends:
        c.wait_send()
    for q in range(low, peers):
        forward(q).wait_send()


def fused(iterate, source, diffusivity):
    peers = lax.axis_size("tm")
    ny, nx = iterate.shape[-2:]
    depth = peers + SWEEPS

    def buffer(*lead):
        return pltpu.VMEM(lead + (ny, nx), jnp.float32)

    dma = pltpu.SemaphoreType.DMA
    shape = pltpu.VMEM(iterate.shape, jnp.float32)
    vmem = pl.BlockSpec(memory_space=pltpu.VMEM)
    update, residual, decrease = pl.pallas_call(
        functools.partial(fused_kernel, peers),
        out_shape=(shape, shape, shape),
        in_specs=[pl.BlockSpec(memory_space=pl.ANY)] * 3,
        out_specs=(vmem, vmem, vmem),
        scratch_shapes=[
            buffer(peers),
            buffer(peers),
            buffer(peers),
            buffer(peers),
            buffer(),
            buffer(peers),
            buffer(peers, 2),
            buffer(peers),
            buffer(peers, 2),
            buffer(peers, 2),
            buffer(peers, 2),
            buffer(peers),
            buffer(depth, 2),
            buffer(depth, 2),
            buffer(SWEEPS, depth + 1, 2),
            buffer(peers, 2),
            buffer(peers, 2),
            buffer(peers, 2),
            buffer(peers, 2),
            pltpu.VMEM((2, nx), jnp.float32),
            pltpu.VMEM((2 * peers, 2, nx), jnp.float32),
            dma((3,)),
            dma,
            dma,
            dma,
            dma,
            dma((peers, 2)),
            dma((peers, 2)),
            dma((peers,)),
            dma((peers,)),
            dma((peers,)),
            dma((peers,)),
            dma((peers,)),
            dma((peers,)),
            dma((peers,)),
            dma((peers,)),
            dma((peers,)),
            dma((peers,)),
            dma((2 * peers,)),
            dma((2 * peers,)),
        ],
        compiler_params=pltpu.CompilerParams(collective_id=0, has_side_effects=True),
    )(iterate, source, diffusivity)
    return iterate + update, residual - decrease


def on_device_any(iterate, source, diffusivity):
    steps, planes, ny, nx = iterate.shape
    peers = lax.axis_size("tm")
    fits = (
        steps == 1
        and planes == peers
        and peers % 2 == 0
        and lax.axis_size("space") == 2
        and planes >= SWEEPS
        and ny % 8 == 0
        and nx % 128 == 0
    )
    return (fused if fits else on_device)(iterate, source, diffusivity)


def solution(mesh):
    in_specs = (
        P(("groups", "tm"), "space", None, None),
        P(("groups", "tm"), "space", None, None),
        P(("groups", "space"), None, None),
    )
    out_specs = (P(("groups", "tm"), "space", None, None), P(("groups", "tm"), "space", None, None))
    return jax.shard_map(
        on_device_any, mesh=mesh, in_specs=in_specs, out_specs=out_specs, check_vma=False
    )
```

```python
import functools
import math

import jax
import jax.numpy as jnp
from jax import lax
from jax.experimental import pallas as pl
from jax.experimental.pallas import tpu as pltpu
from jax.sharding import PartitionSpec as P

SWEEPS = 6


frac_order = 0.3
step_length = 0.01
gamma_factor = 0.9086387328532904


def with_halo(value, sides, width):
    for axis, dim in sides:
        peers, length = (lax.axis_size(axis), value.shape[dim])
        up = [(i, (i + 1) % peers) for i in range(peers - 1)]
        down = [(j, i) for i, j in up]
        last = lax.slice_in_dim(value, length - width, length, axis=dim)
        first = lax.slice_in_dim(value, 0, width, axis=dim)
        before = lax.ppermute(last, axis, up)
        after = lax.ppermute(first, axis, down)
        value = jnp.concatenate([before, value, after], axis=dim)
    return value


def history_weights(lags):
    scale = 1.0 / (step_length**frac_order * gamma_factor)
    power = 1.0 - frac_order
    safe = jnp.maximum(lags, 0.0)
    upper = (safe + 1.0) ** power - safe**power
    lower = jnp.where(safe >= 1.0, safe**power - jnp.maximum(safe - 1.0, 0.0) ** power, 0.0)
    return jnp.where(lags >= 0.0, (upper - lower) * scale, 0.0)


def circulant_spectrum(freqs, total):
    lags = jnp.arange(total, dtype=jnp.int32)
    first = jnp.where(lags < total // 2, history_weights(lags.astype(jnp.float32)), 0.0)
    phase = (freqs[:, None] * lags[None, :] % total).astype(jnp.float32) * (2.0 * math.pi / total)
    real_part = jnp.sum(first[None, :] * jnp.cos(phase), axis=1)
    imag_part = -jnp.sum(first[None, :] * jnp.sin(phase), axis=1)
    return (real_part, imag_part)


def fourier_tables(total):
    index = jnp.arange(total, dtype=jnp.int32)
    phase = (index[:, None] * index[None, :] % total).astype(jnp.float32) * (2.0 * math.pi / total)
    return (jnp.cos(phase), jnp.sin(phase))


def neighbour_sum(padded):
    inner = padded[..., 1:-1, :, :]
    result = padded[..., 2:, :, :] + padded[..., :-2, :, :]
    along_y = jnp.pad(inner, [(0, 0)] * (inner.ndim - 2) + [(1, 1), (0, 0)])
    result = result + along_y[..., 2:, :] + along_y[..., :-2, :]
    along_x = jnp.pad(inner, [(0, 0)] * (inner.ndim - 1) + [(1, 1)])
    return result + along_x[..., 2:] + along_x[..., :-2]


def jacobi_step(
    spec_re, spec_im, sol_re, sol_im, stiff_re, stiff_im, lam_re, lam_im, inv_re, inv_im
):
    res_re = spec_re - (lam_re * sol_re - lam_im * sol_im) - stiff_re
    res_im = spec_im - (lam_re * sol_im + lam_im * sol_re) - stiff_im
    return (
        sol_re + (res_re * inv_re - res_im * inv_im),
        sol_im + (res_re * inv_im + res_im * inv_re),
    )


def stiffness_pair(sol_re, sol_im, diffusivity):
    stacked = jnp.stack([sol_re, sol_im])
    padded = with_halo(stacked, (("space", 2),), 1)
    stiff = diffusivity * (6.0 * stacked - neighbour_sum(padded))
    return (stiff[0], stiff[1])


def time_product(matrix, field):
    return jnp.dot(matrix, field, precision=lax.Precision.HIGHEST)


def inner_products(residual, image):
    return lax.psum((jnp.sum(residual * image), jnp.sum(image * image)), ("tm", "space"))


def on_device(iterate, source, diffusivity):
    steps_here = iterate.shape[0]
    slab_shape = iterate.shape
    cells = slab_shape[1] * slab_shape[2] * slab_shape[3]
    total = steps_here * lax.axis_size("tm")
    my_times = lax.axis_index("tm") * steps_here + jnp.arange(steps_here, dtype=jnp.int32)
    times = jnp.arange(total, dtype=jnp.int32)
    toeplitz = history_weights((times[:, None] - times[None, :]).astype(jnp.float32))
    cos_table, sin_table = fourier_tables(total)
    padded = with_halo(iterate, (("space", 1),), 1)
    stiff_iter = diffusivity * (6.0 * iterate - neighbour_sum(padded))
    flat_iter = iterate.reshape(steps_here, cells)
    flat_source = source.reshape(steps_here, cells)
    flat_stiff = stiff_iter.reshape(steps_here, cells)
    iter_cols, source_cols, stiff_cols = (
        lax.all_to_all(flat_iter, "tm", split_axis=1, concat_axis=0, tiled=True),
        lax.all_to_all(flat_source, "tm", split_axis=1, concat_axis=0, tiled=True),
        lax.all_to_all(flat_stiff, "tm", split_axis=1, concat_axis=0, tiled=True),
    )
    residual = source_cols - time_product(toeplitz, iter_cols) - stiff_cols
    spec_re = time_product(cos_table, residual)
    spec_im = -time_product(sin_table, residual)
    spec_re, spec_im = (
        lax.all_to_all(spec_re, "tm", split_axis=0, concat_axis=1, tiled=True),
        lax.all_to_all(spec_im, "tm", split_axis=0, concat_axis=1, tiled=True),
    )
    spec_re = spec_re.reshape(slab_shape)
    spec_im = spec_im.reshape(slab_shape)
    lam_re, lam_im = circulant_spectrum(my_times, total)
    lam_re = lam_re[:, None, None, None]
    lam_im = lam_im[:, None, None, None]
    diag_re = lam_re + 6.0 * diffusivity
    denom = diag_re * diag_re + lam_im * lam_im
    inv_re = diag_re / denom
    inv_im = -lam_im / denom
    sol_re = spec_re * inv_re - spec_im * inv_im
    sol_im = spec_re * inv_im + spec_im * inv_re
    for sweep in range(SWEEPS - 1):
        stiff_re, stiff_im = stiffness_pair(sol_re, sol_im, diffusivity)
        sol_re, sol_im = jacobi_step(
            spec_re, spec_im, sol_re, sol_im, stiff_re, stiff_im, lam_re, lam_im, inv_re, inv_im
        )
    stiff_re, stiff_im = stiffness_pair(sol_re, sol_im, diffusivity)
    sol_re, sol_im, stiff_re, stiff_im = (
        lax.all_to_all(
            sol_re.reshape(steps_here, cells), "tm", split_axis=1, concat_axis=0, tiled=True
        ),
        lax.all_to_all(
            sol_im.reshape(steps_here, cells), "tm", split_axis=1, concat_axis=0, tiled=True
        ),
        lax.all_to_all(
            stiff_re.reshape(steps_here, cells), "tm", split_axis=1, concat_axis=0, tiled=True
        ),
        lax.all_to_all(
            stiff_im.reshape(steps_here, cells), "tm", split_axis=1, concat_axis=0, tiled=True
        ),
    )
    correction = (time_product(cos_table, sol_re) - time_product(sin_table, sol_im)) / total
    stiff_time = (time_product(cos_table, stiff_re) - time_product(sin_table, stiff_im)) / total
    image = time_product(toeplitz, correction) + stiff_time
    inner_ri, inner_ii = inner_products(residual, image)
    step = inner_ri / inner_ii
    new_residual = residual - step * image
    correction_slab, residual_back = (
        lax.all_to_all(correction, "tm", split_axis=0, concat_axis=1, tiled=True),
        lax.all_to_all(new_residual, "tm", split_axis=0, concat_axis=1, tiled=True),
    )
    new_iterate = iterate + step * correction_slab.reshape(slab_shape)
    return (new_iterate, residual_back.reshape(slab_shape))


def constants(total):
    scale = 1.0 / (step_length**frac_order * gamma_factor)
    power = 1.0 - frac_order
    b = [(k + 1.0) ** power - float(k) ** power for k in range(total)]
    d = [scale * (b[k] - (b[k - 1] if k else 0.0)) for k in range(total)]
    angle = [2.0 * math.pi * i / total for i in range(total)]
    cos = [math.cos(a) for a in angle]
    sin = [math.sin(a) for a in angle]
    half = total // 2
    lam_re = [sum(d[k] * cos[j * k % total] for k in range(half)) for j in range(total)]
    lam_im = [-sum(d[k] * sin[j * k % total] for k in range(half)) for j in range(total)]
    return d, cos, sin, lam_re, lam_im


def weighted(terms):
    result = None
    for weight, value in terms:
        if abs(weight) < 1e-9:
            continue
        if result is None:
            result = value if abs(weight - 1.0) < 1e-9 else weight * value
        elif abs(weight - 1.0) < 1e-9:
            result = result + value
        elif abs(weight + 1.0) < 1e-9:
            result = result - value
        else:
            result = result + weight * value
    return result


def pick(index, values):
    result = jnp.float32(values[0])
    for i in range(1, len(values)):
        result = jnp.where(index == i, jnp.float32(values[i]), result)
    return result


def exchange_order(me, peers):
    if peers & (peers - 1):
        return [lax.rem(me + i, peers) for i in range(1, peers)]
    bits = range(peers.bit_length() - 1)
    result = []
    for mask in range(peers - 1, 0, -1):
        partner = 0
        for b in bits:
            digit = lax.rem(me // (1 << b), 2)
            partner = partner + ((1 - digit) if mask >> b & 1 else digit) * (1 << b)
        result.append(partner)
    return result


def fused_kernel(
    peers,
    u_hbm,
    f_hbm,
    k_hbm,
    x_out,
    r_out,
    dr_out,
    u,
    f,
    kap,
    kap_far,
    u_halo,
    wbuf,
    got_uw,
    res,
    spec,
    got_spec,
    far_spec,
    got_res,
    gain,
    hop,
    sols,
    xy,
    got_xy,
    ci,
    got_ci,
    part,
    got_part,
    load_sem,
    halo_send,
    halo_recv,
    kap_send,
    kap_recv,
    uw_send,
    uw_recv,
    spec_send,
    spec_recv,
    far_send,
    far_recv,
    res_send,
    res_recv,
    xy_send,
    xy_recv,
    ci_send,
    ci_recv,
    part_send,
    part_recv,
):
    me = lax.axis_index("tm")
    side = lax.axis_index("space")
    ny, nx = u.shape[-2:]
    reach = SWEEPS
    low = peers - reach
    d, cos, sin, lam_re, lam_im = constants(peers)
    half = peers // 2
    start = peers // 4

    def slot_of(k):
        return lax.rem(k - start + peers, half)

    slot = slot_of(me)
    others = exchange_order(me, peers)
    mesh_type = pl.DeviceIdType.MESH

    def works(k):
        return jnp.logical_and(k >= start, k < start + half)

    def plane(q):
        return side * (peers - 1) + q * (1 - 2 * side)

    def at_tm(k):
        return {"tm": k}

    across = {"space": 1 - side}

    def diagonal(k):
        return {"tm": k, "space": 1 - side}

    def copy(src, dst, send, recv, device):
        return pltpu.make_async_remote_copy(
            src_ref=src,
            dst_ref=dst,
            send_sem=send,
            recv_sem=recv,
            device_id=device,
            device_id_type=mesh_type,
        )

    loads = [
        pltpu.make_async_copy(a, b, load_sem.at[i])
        for i, (a, b) in enumerate(((u_hbm.at[0], u), (k_hbm, kap), (f_hbm.at[0], f)))
    ]
    for load in loads:
        load.start()
    barrier = pltpu.get_barrier_semaphore()
    for k in others:
        pl.semaphore_signal(barrier, inc=1, device_id=at_tm(k), device_id_type=mesh_type)
    pl.semaphore_signal(barrier, inc=1, device_id=across, device_id_type=mesh_type)
    loads[0].wait()
    loads[1].wait()
    loads[2].wait()

    rows = lax.broadcasted_iota(jnp.int32, (ny, nx), 0)
    lanes = lax.broadcasted_iota(jnp.int32, (ny, nx), 1)
    not_top = rows > 0
    not_bottom = rows < ny - 1
    not_left = lanes > 0
    not_right = lanes < nx - 1

    def in_plane(v):
        y = jnp.where(not_top, pltpu.roll(v, 1, 0), 0.0) + jnp.where(
            not_bottom, pltpu.roll(v, ny - 1, 0), 0.0
        )
        x = jnp.where(not_left, pltpu.roll(v, 1, 1), 0.0) + jnp.where(
            not_right, pltpu.roll(v, nx - 1, 1), 0.0
        )
        return y + x

    pl.semaphore_wait(barrier, peers)
    halo = copy(u.at[plane(peers - 1)], u_halo, halo_send, halo_recv, across)
    halo.start()
    sends = [halo]
    for k in others:
        c = copy(
            u.at[plane(k)], got_uw.at[me, 0], uw_send.at[k, 0], uw_recv.at[me, 0], at_tm(k)
        )
        c.start()
        sends.append(c)
    kap_copy = copy(kap, kap_far, kap_send, kap_recv, across)
    kap_copy.start()
    sends.append(kap_copy)

    def stiff_of_iterate(q, after):
        value = u[plane(q)]
        total = in_plane(value) + after
        if q > 0:
            total = total + u[plane(q - 1)]
        wbuf[q] = f[plane(q)] - kap[plane(q)] * (6.0 * value - total)

    for q in range(peers - 1):
        stiff_of_iterate(q, u[plane(q + 1)])
    halo.wait_recv()
    stiff_of_iterate(peers - 1, u_halo[...])
    for k in others:
        c = copy(wbuf.at[k], got_uw.at[me, 1], uw_send.at[k, 1], uw_recv.at[me, 1], at_tm(k))
        c.start()
        sends.append(c)
    got_uw[me, 0] = u[plane(me)]
    got_uw[me, 1] = wbuf[me]

    first_lam = pick(slot, lam_re[:half])
    second_lam = pick(slot, [lam_re[half]] + lam_re[1:half])
    my_im = pick(slot, [0.0] + lam_im[1:half])
    kap_copy.wait_recv()
    depth = peers + reach
    for q in range(depth):
        kappa = kap[plane(q)] if q < peers else kap_far[(1 - side) * (peers - 1) + (2 * peers - 1 - q) * (2 * side - 1)]
        diag = first_lam + 6.0 * kappa
        inverse = 1.0 / (diag * diag + my_im * my_im)
        other = second_lam + 6.0 * kappa
        g_first = diag * inverse
        g_second = other / (other * other + my_im * my_im)
        g_cross = -my_im * inverse
        gain[q, 0] = g_first
        gain[q, 1] = g_second
        gain[q, 2] = g_cross
        hop[q, 0] = g_first * kappa
        hop[q, 1] = g_second * kappa
        hop[q, 2] = g_cross * kappa
    zero = jnp.zeros((ny, nx), jnp.float32)
    for level in range(SWEEPS):
        sols[level, 0, 0] = zero
        sols[level, 0, 1] = zero

    for k in others:
        for i in range(2):
            copy(
                wbuf.at[k], got_uw.at[k, i], uw_send.at[k, i], uw_recv.at[k, i], at_tm(k)
            ).wait_recv()
    residual = []
    for n in range(peers):
        history = weighted([(d[n - m], got_uw[m, 0]) for m in range(n + 1)])
        value = got_uw[n, 1] - history
        res[n] = value
        residual.append(value)
    spec[0, 0] = weighted([(1.0, residual[n]) for n in range(peers)])
    spec[0, 1] = weighted([(cos[half * n % peers], residual[n]) for n in range(peers)])
    for j in range(1, half):
        spec[j, 0] = weighted([(cos[j * n % peers], residual[n]) for n in range(peers)])
        spec[j, 1] = weighted([(-sin[j * n % peers], residual[n]) for n in range(peers)])

    def spec_copy(k, source):
        return copy(
            spec.at[slot_of(k)], got_spec.at[source], spec_send.at[k], spec_recv.at[source], at_tm(k)
        )

    def forward(q):
        return copy(got_spec.at[q], far_spec.at[q], far_send.at[q], far_recv.at[q], across)

    for k in others:

        @pl.when(works(k))
        def _():
            spec_copy(k, me).start()

    @pl.when(works(me))
    def _():
        got_spec[me] = spec[slot]

        @pl.when(me >= low)
        def _():
            copy(
                spec.at[slot], far_spec.at[me], far_send.at[me], far_recv.at[me], across
            ).start()

        for k in others:
            copy(
                spec.at[0], got_spec.at[k], spec_send.at[k], spec_recv.at[k], at_tm(k)
            ).wait_recv()

            @pl.when(k >= low)
            def _():
                forward(k).start()

    for k in others:
        c = copy(res.at[k], got_res.at[me], res_send.at[k], res_recv.at[me], at_tm(k))
        c.start()
        sends.append(c)
    got_res[me] = res[me]
    def first_solution(q, s):
        cross = gain[q, 2]
        sols[0, q + 1, 0] = s[0] * gain[q, 0] - s[1] * cross
        sols[0, q + 1, 1] = s[1] * gain[q, 1] + s[0] * cross

    def neighbours(buffer, q, i):
        return buffer[q, i] + buffer[q + 2, i] + in_plane(buffer[q + 1, i])

    def sweep_plane(level, q):
        before = sols.at[level - 1]
        n_re = neighbours(before, q, 0)
        n_im = neighbours(before, q, 1)
        cross = hop[q, 2]
        sols[level, q + 1, 0] = sols[0, q + 1, 0] + (hop[q, 0] * n_re - cross * n_im)
        sols[level, q + 1, 1] = sols[0, q + 1, 1] + (hop[q, 1] * n_im + cross * n_re)

    def xy_copy(k, source):
        return copy(xy.at[k], got_xy.at[source], xy_send.at[k], xy_recv.at[source], at_tm(k))

    @pl.when(works(me))
    def _():
        for q in range(peers):
            first_solution(q, got_spec[q])
        for level in range(1, SWEEPS):
            lax.fori_loop(0, peers - level, lambda q, c, level=level: sweep_plane(level, q), None, unroll=True)
        for q in range(low, peers):
            forward(q).wait_recv()
        for q in range(peers, depth):
            first_solution(q, far_spec[2 * peers - 1 - q])
        for level in range(1, SWEEPS):
            lax.fori_loop(
                peers - level,
                depth - level,
                lambda q, c, level=level: sweep_plane(level, q),
                None,
                unroll=True,
            )
        now = sols.at[SWEEPS - 1]

        def stiff_plane(q, carry):
            kappa = kap[plane(q)]
            for i in range(2):
                value = now[q + 1, i]
                xy[q, i] = value
                xy[q, 2 + i] = kappa * (6.0 * value - neighbours(now, q, i))
            return carry

        lax.fori_loop(0, peers, stiff_plane, 0, unroll=True)
        for k in others:
            xy_copy(k, slot).start()
        got_xy[slot] = xy[me]

    for k in others:

        @pl.when(works(k))
        def _():
            xy_copy(k, slot_of(k)).wait_recv()

    inv = 1.0 / peers
    corrections = []

    def inverse_terms(n, i):
        terms = [(inv, got_xy[0, i]), (inv * cos[n * half % peers], got_xy[0, i + 1])]
        for j in range(1, half):
            terms.append((2.0 * inv * cos[n * j % peers], got_xy[j, i]))
            terms.append((-2.0 * inv * sin[n * j % peers], got_xy[j, i + 1]))
        return terms

    for n in range(peers):
        value = weighted(inverse_terms(n, 0))
        ci[n, 0] = value
        corrections.append(value)
    inner_ri = zero
    inner_ii = zero
    for n in range(peers):
        terms = inverse_terms(n, 2)
        image = weighted(terms + [(d[n - m], corrections[m]) for m in range(n + 1)])
        ci[n, 1] = image
        inner_ri = inner_ri + res[n] * image
        inner_ii = inner_ii + image * image
    part[0:1] = jnp.sum(inner_ri, axis=0, keepdims=True)
    part[1:2] = jnp.sum(inner_ii, axis=0, keepdims=True)
    mine = side * peers + me
    opposite = (1 - side) * peers

    def part_copy(slot, source, device):
        return copy(part, got_part.at[source], part_send.at[slot], part_recv.at[source], device)

    for k in others:
        for place, device in ((side * peers + k, at_tm(k)), (opposite + k, diagonal(k))):
            c = part_copy(place, mine, device)
            c.start()
            sends.append(c)
    c = part_copy(opposite + me, mine, across)
    c.start()
    sends.append(c)
    for k in others:
        c = copy(ci.at[k], got_ci.at[me], ci_send.at[k], ci_recv.at[me], at_tm(k))
        c.start()
        sends.append(c)
    got_ci[me] = ci[me]
    got_part[mine] = part[...]
    for k in others:
        copy(res.at[k], got_res.at[k], res_send.at[k], res_recv.at[k], at_tm(k)).wait_recv()
    for q in range(peers):
        r_out[0, plane(q)] = got_res[q]
    for k in others:
        part_copy(side * peers + k, side * peers + k, at_tm(k)).wait_recv()
        part_copy(opposite + k, opposite + k, diagonal(k)).wait_recv()
    part_copy(opposite + me, opposite + me, across).wait_recv()
    sums = got_part[0]
    for i in range(1, 2 * peers):
        sums = sums + got_part[i]
    sums = jnp.sum(sums, axis=1, keepdims=True)
    step = sums[0:1] / sums[1:2]
    for k in others:
        copy(ci.at[k], got_ci.at[k], ci_send.at[k], ci_recv.at[k], at_tm(k)).wait_recv()
    for q in range(peers):
        x_out[0, plane(q)] = step * got_ci[q, 0]
        dr_out[0, plane(q)] = step * got_ci[q, 1]
    for c in sends:
        c.wait_send()
    for k in others:

        @pl.when(works(k))
        def _():
            spec_copy(k, me).wait_send()

    @pl.when(works(me))
    def _():
        for q in range(low, peers):
            forward(q).wait_send()
        for k in others:
            xy_copy(k, slot).wait_send()


def fused(iterate, source, diffusivity):
    peers = lax.axis_size("tm")
    ny, nx = iterate.shape[-2:]
    depth = peers + SWEEPS

    def buffer(*lead):
        return pltpu.VMEM(lead + (ny, nx), jnp.float32)

    dma = pltpu.SemaphoreType.DMA
    shape = pltpu.VMEM(iterate.shape, jnp.float32)
    vmem = pl.BlockSpec(memory_space=pltpu.VMEM)
    update, residual, decrease = pl.pallas_call(
        functools.partial(fused_kernel, peers),
        out_shape=(shape, shape, shape),
        in_specs=[pl.BlockSpec(memory_space=pl.ANY)] * 3,
        out_specs=(vmem, vmem, vmem),
        scratch_shapes=[
            buffer(peers),
            buffer(peers),
            buffer(peers),
            buffer(peers),
            buffer(),
            buffer(peers),
            buffer(peers, 2),
            buffer(peers),
            buffer(peers // 2, 2),
            buffer(peers, 2),
            buffer(peers, 2),
            buffer(peers),
            buffer(depth, 3),
            buffer(depth, 3),
            buffer(SWEEPS, depth + 1, 2),
            buffer(peers, 4),
            buffer(peers // 2, 4),
            buffer(peers, 2),
            buffer(peers, 2),
            pltpu.VMEM((2, nx), jnp.float32),
            pltpu.VMEM((2 * peers, 2, nx), jnp.float32),
            dma((3,)),
            dma,
            dma,
            dma,
            dma,
            dma((peers, 2)),
            dma((peers, 2)),
            dma((peers,)),
            dma((peers,)),
            dma((peers,)),
            dma((peers,)),
            dma((peers,)),
            dma((peers,)),
            dma((peers,)),
            dma((peers,)),
            dma((peers,)),
            dma((peers,)),
            dma((2 * peers,)),
            dma((2 * peers,)),
        ],
        compiler_params=pltpu.CompilerParams(collective_id=0, has_side_effects=True),
    )(iterate, source, diffusivity)
    return iterate + update, residual - decrease


def on_device_any(iterate, source, diffusivity):
    steps, planes, ny, nx = iterate.shape
    peers = lax.axis_size("tm")
    fits = (
        steps == 1
        and planes == peers
        and peers % 4 == 0
        and lax.axis_size("space") == 2
        and planes >= SWEEPS
        and ny % 8 == 0
        and nx % 128 == 0
    )
    return (fused if fits else on_device)(iterate, source, diffusivity)


def solution(mesh):
    in_specs = (
        P(("groups", "tm"), "space", None, None),
        P(("groups", "tm"), "space", None, None),
        P(("groups", "space"), None, None),
    )
    out_specs = (P(("groups", "tm"), "space", None, None), P(("groups", "tm"), "space", None, None))
    return jax.shard_map(
        on_device_any, mesh=mesh, in_specs=in_specs, out_specs=out_specs, check_vma=False
    )
```
